32 devices in a mesh: graph: 8 (over z, y), member: 4 (over x, core).
Axes of the slice: x: 2, y: 2, z: 4, core: 2. Of those that a mesh axis runs over, the one named last changes fastest.
Arguments:
- node_latents: bfloat16 [16, 1024, 512], P('member', 'graph'), may hold values from -6 to 6
- edge_latents: bfloat16 [6144, 512], P('graph'), may hold values from -6 to 6
- neighbours: int32 [8, 4], P('graph'), may hold values from 0 to 7, as said below
- edge_source: int32 [8, 768], P('graph'), may hold values from 0 to 639, as said below
- edge_dest: int32 [8, 768], P('graph'), may hold values from 0 to 127, as said below
- edge_count: int32 [8], P('graph'), may hold values from 153 to 768, as said below
- edge_in: bfloat16 [1, 3, 512, 512], replicated, may hold values from -0.15625 to 0.15625
- edge_out: bfloat16 [1, 512, 512], replicated, may hold values from -0.25 to 0.25
- node_in: bfloat16 [1, 2, 512, 512], replicated, may hold values from -0.1875 to 0.1875
- node_out: bfloat16 [1, 512, 512], replicated, may hold values from -0.25 to 0.25
- biases: float32 [1, 4, 512], replicated, may hold values from -3 to 3
- gains: float32 [1, 2, 512], replicated, may hold values from 0.25 to 1.75
Outputs:
- ens_mean: bfloat16 [1024, 512], P('graph')
- ens_spread: bfloat16 [1024, 512], P('graph')
The draws below stay inside these ranges and needn't reach their ends.
Inputs may be any that keep to these rules, and one draw needn't show every extreme that they name: `neighbours`: row b lists 4 distinct blocks other than b, each within 3 blocks of b along the closed order of blocks (numbers taken modulo 8). `edge_source`: among the live edge slots of one block, at most 32 distinct sender nodes lie in any one listed block, and exactly 32 in one of them. `edge_dest`: every node receives at least one live edge slot of its block. `edge_count`: some block has all 768 slots live.
All inputs are finite; a program needn't handle non-finite values.
Results may differ from the reference program's by a relative error of at most 0.006.
Values may be sent and summed in bfloat16 or wider, within the bound.
A program may use at most 64 MiB of HBM per device.

```python
import jax
import jax.numpy as jnp
from jax import lax

L = 512
BLK = 128
EDGE_DEV = 768
NBRS = 4
RADIUS = 3
CAP = 32
LAYERS = 1
BLOCKS = 8
NODES = 1024
EDGES = 6144
MEMBERS = 16


def graph_tables(key):
    folded = jax.random.fold_in(key, 4242)
    keys = jax.random.split(folded, 8)
    blocks = jnp.arange(BLOCKS, dtype=jnp.int32)
    candidate_ids = jnp.arange(2 * RADIUS, dtype=jnp.int32)
    candidates = jnp.where(candidate_ids < RADIUS, candidate_ids + 1, RADIUS - 1 - candidate_ids)
    order = jax.vmap(lambda subkey: jax.random.permutation(subkey, 2 * RADIUS))(jax.random.split(keys[0], BLOCKS))[:, :NBRS]
    offsets = candidates[order]
    neighbours = (blocks[:, None] + offsets) % BLOCKS
    counts = EDGE_DEV // (1 + jax.random.randint(keys[1], (BLOCKS,), 0, 5))
    busiest = jax.random.randint(keys[2], (), 0, BLOCKS)
    counts = jnp.where(blocks == busiest, EDGE_DEV, counts)
    needed = jax.random.randint(keys[3], (BLOCKS, NBRS), CAP // 2, CAP + 1)
    widest = jax.random.randint(keys[4], (BLOCKS,), 0, NBRS)
    needed = jnp.where(jnp.arange(NBRS, dtype=jnp.int32)[None, :] == widest[:, None], CAP, needed)
    chosen = jax.vmap(lambda subkey: jax.random.permutation(subkey, BLK))(jax.random.split(keys[5], BLOCKS * NBRS))
    chosen = chosen.reshape(BLOCKS, NBRS, BLK)[:, :, :CAP].reshape(BLOCKS, NBRS * CAP)
    slots = jnp.arange(EDGE_DEV, dtype=jnp.int32)
    first_slot = jnp.minimum(slots // CAP, NBRS - 1)
    first_rank = slots % CAP
    in_first = (slots < NBRS * CAP)[None, :]
    random_bits = jax.random.randint(keys[6], (4, BLOCKS, EDGE_DEV), 0, 1 << 20)
    slot_pick = jnp.where(in_first, first_slot[None, :], random_bits[0] % NBRS)
    need_at = jnp.take_along_axis(needed, slot_pick, axis=1)
    rank_pick = jnp.where(in_first, first_rank[None, :], random_bits[1] % need_at)
    remote = jnp.where(in_first, first_rank[None, :] < need_at, random_bits[2] % 4 == 0)
    node_pick = jnp.take_along_axis(chosen, slot_pick * CAP + rank_pick, axis=1)
    own_node = random_bits[3] % BLK
    source = jnp.where(remote, slot_pick * BLK + node_pick, NBRS * BLK + own_node)
    receivers = jax.vmap(lambda subkey: jax.random.permutation(subkey, BLK))(jax.random.split(keys[7], BLOCKS))
    dest = jnp.take(receivers, slots % BLK, axis=1)
    return (neighbours.astype(jnp.int32), source.astype(jnp.int32), dest.astype(jnp.int32), counts.astype(jnp.int32))


def draw_neighbours(key, part):
    return graph_tables(key)[0]


def draw_edge_source(key, part):
    return graph_tables(key)[1]


def draw_edge_dest(key, part):
    return graph_tables(key)[2]


def draw_edge_count(key, part):
    return graph_tables(key)[3]


def level_of(stream_key, extent, pieces, least, top_value):
    factor_of, own = 1.0, jax.random.fold_in(stream_key, 6)
    for position, blocks in pieces:
        heights = jnp.exp(jax.random.uniform(jax.random.fold_in(own, position), (blocks,), jnp.float32, least / len(pieces), top_value / len(pieces)))
        factor_of = factor_of * jnp.repeat(heights, extent[position] // blocks).reshape([-1 if axis == position else 1 for axis in range(len(extent))])
    return factor_of


def normal_values(stream_key, shape, scale, limit, shards=(), held_as=jnp.bfloat16):
    factor_of = level_of(stream_key, shape, shards, -0.22, 0.18) if shards else 1.0
    entries = jax.random.normal(stream_key, shape, jnp.float32) * scale * factor_of
    return jnp.minimum(jnp.maximum(entries, -limit), limit).astype(held_as)


def setup_inputs(seed: int = 0) -> dict:
    key_of = jax.random.split(jax.random.key(seed), 13)
    node_latents = normal_values(key_of[0], (MEMBERS, NODES, L), 1.0, 6.0, ((0, 4), (1, 8)))
    edge_latents = normal_values(key_of[1], (EDGES, L), 1.0, 6.0, ((0, 8),))
    neighbours = draw_neighbours(jax.random.fold_in(key_of[12], 71), 0)
    edge_source = draw_edge_source(jax.random.fold_in(key_of[12], 71), 0)
    edge_dest = draw_edge_dest(jax.random.fold_in(key_of[12], 71), 0)
    edge_count = draw_edge_count(jax.random.fold_in(key_of[12], 71), 0)
    edge_in = normal_values(key_of[6], (LAYERS, 3, L, L), (3 * L) ** -0.5, 0.15625)
    edge_out = normal_values(key_of[7], (LAYERS, L, L), L ** -0.5, 0.25)
    node_in = normal_values(key_of[8], (LAYERS, 2, L, L), (2 * L) ** -0.5, 0.1875)
    node_out = normal_values(key_of[9], (LAYERS, L, L), L ** -0.5, 0.25)
    biases = normal_values(key_of[10], (LAYERS, 4, L), 0.5, 3.0, (), jnp.float32)
    gains = jnp.clip(1.0 + 0.15 * jax.random.normal(key_of[11], (LAYERS, 2, L), jnp.float32), 0.25, 1.75)
    return dict(node_latents=node_latents, edge_latents=edge_latents, neighbours=neighbours, edge_source=edge_source, edge_dest=edge_dest, edge_count=edge_count, edge_in=edge_in, edge_out=edge_out, node_in=node_in, node_out=node_out, biases=biases, gains=gains)


def layer_norm(values, gain):
    centre = lax.optimization_barrier(jnp.mean(values, axis=-1, keepdims=True))
    centered = values - centre
    variance = lax.optimization_barrier(jnp.mean(centered * centered, axis=-1, keepdims=True))
    return centered * lax.rsqrt(variance + 1e-05) * gain

def reference(node_latents, edge_latents, neighbours, edge_source, edge_dest, edge_count, edge_in, edge_out, node_in, node_out, biases, gains):
    blocks = jnp.arange(BLOCKS, dtype=jnp.int32)[:, None]
    src_slot = edge_source // BLK
    src_node = edge_source % BLK
    listed = jnp.take_along_axis(neighbours, jnp.minimum(src_slot, NBRS - 1), axis=1)
    owner = jnp.where(src_slot == NBRS, blocks, listed)
    src_global = (owner * BLK + src_node).reshape(-1).astype(jnp.int32)
    dst_global = (blocks * BLK + edge_dest).reshape(-1).astype(jnp.int32)
    is_live = (jnp.arange(EDGE_DEV, dtype=jnp.int32)[None, :] < edge_count[:, None]).reshape(-1)

    def one_member(state):
        edge_state = edge_latents
        for layer_id in range(LAYERS):
            sender_proj = jnp.dot(state, edge_in[layer_id, 1], preferred_element_type=jnp.float32).astype(jnp.bfloat16)
            receiver_proj = jnp.dot(state, edge_in[layer_id, 2], preferred_element_type=jnp.float32)
            hidden = jnp.dot(edge_state, edge_in[layer_id, 0], preferred_element_type=jnp.float32)
            hidden = hidden + sender_proj[src_global].astype(jnp.float32) + receiver_proj[dst_global] + biases[layer_id, 0]
            activated = jax.nn.silu(hidden).astype(jnp.bfloat16)
            mixed = jnp.dot(activated, edge_out[layer_id], preferred_element_type=jnp.float32) + biases[layer_id, 1]
            edge_state = (edge_state.astype(jnp.float32) + layer_norm(mixed, gains[layer_id, 0])).astype(jnp.bfloat16)
            masked = jnp.where(is_live[:, None], edge_state.astype(jnp.float32), jnp.float32(0.0))
            gathered = jax.ops.segment_sum(masked, dst_global, num_segments=NODES).astype(jnp.bfloat16)
            node_hidden = jnp.dot(state, node_in[layer_id, 0], preferred_element_type=jnp.float32)
            node_hidden = node_hidden + jnp.dot(gathered, node_in[layer_id, 1], preferred_element_type=jnp.float32) + biases[layer_id, 2]
            node_act = jax.nn.silu(node_hidden).astype(jnp.bfloat16)
            node_mixed = jnp.dot(node_act, node_out[layer_id], preferred_element_type=jnp.float32) + biases[layer_id, 3]
            state = (state.astype(jnp.float32) + layer_norm(node_mixed, gains[layer_id, 1])).astype(jnp.bfloat16)
        return state
    finals = lax.map(one_member, node_latents).astype(jnp.float32)
    centre = lax.optimization_barrier(jnp.sum(finals, axis=0)) / MEMBERS
    deviation = finals - centre
    spread = jnp.sqrt(lax.optimization_barrier(jnp.sum(deviation * deviation, axis=0)) / MEMBERS)
    return (centre.astype(jnp.bfloat16), spread.astype(jnp.bfloat16))
```

```python
import functools

import jax
import jax.numpy as jnp
from jax import lax
from jax.experimental import pallas as pl
from jax.experimental.pallas import tpu as pltpu
from jax.sharding import PartitionSpec as P

RADIUS = 3
CAP = 32
REACH = 2 * RADIUS
MESH = pl.DeviceIdType.MESH
F32 = jnp.float32
BF16 = jnp.bfloat16


def dot(a, b):
    return jnp.dot(a, b, preferred_element_type=F32)


def silu(v):
    h = 0.5 * v
    return h * jnp.tanh(h) + h


def layer_norm(values, gain):
    centre = jnp.mean(values, axis=-1, keepdims=True)
    centered = values - centre
    variance = jnp.mean(centered * centered, axis=-1, keepdims=True)
    return centered * lax.rsqrt(variance + 1e-05) * gain


def kernel(
    groups,
    peers,
    nbr_ref,
    count_ref,
    src_ref,
    dst_ref,
    bias_ref,
    gain_ref,
    x_hbm,
    edge_hbm,
    ein_hbm,
    eout_hbm,
    nin_hbm,
    nout_hbm,
    out_ref,
    x,
    edge,
    ein,
    eout,
    nin,
    nout,
    ask,
    asked,
    outbox,
    table,
    hot,
    dest_hot,
    edge_proj,
    node_proj,
    finals,
    inbox,
    load_sem,
    ask_send,
    ask_recv,
    row_send,
    row_recv,
    fin_send,
    fin_recv,
    res_send,
    res_recv,
):
    members, rows, width = x.shape
    slots = edge.shape[0]
    nbrs = nbr_ref.shape[1]
    part = rows // peers
    me_g = lax.axis_index("graph")
    me_m = lax.axis_index("member")
    steps = [r + 1 for r in range(RADIUS)] + [-(r + 1) for r in range(RADIUS)]

    def ahead(step):
        return lax.rem(me_g + step + groups, groups)

    def peer(k):
        return lax.rem(me_m + k, peers)

    loads = [
        pltpu.make_async_copy(s, d, load_sem.at[i])
        for i, (s, d) in enumerate(
            [
                (x_hbm, x),
                (ein_hbm.at[0, 1], ein.at[1]),
                (ein_hbm.at[0, 2], ein.at[2]),
                (edge_hbm, edge),
                (ein_hbm.at[0, 0], ein.at[0]),
                (nin_hbm.at[0], nin),
                (eout_hbm.at[0], eout),
                (nout_hbm.at[0], nout),
            ]
        )
    ]
    for load in loads:
        load.start()

    barrier = pltpu.get_barrier_semaphore()
    for step in steps:
        pl.semaphore_signal(
            barrier, inc=1, device_id=(ahead(step), me_m), device_id_type=MESH
        )
    for k in range(1, peers):
        pl.semaphore_signal(
            barrier, inc=1, device_id=(me_g, peer(k)), device_id_type=MESH
        )

    src = src_ref[...]
    dst = dst_ref[...]
    live = lax.broadcasted_iota(jnp.int32, (1, slots), 1) < count_ref[0]
    slot = jnp.zeros_like(src)
    for k in range(1, nbrs + 1):
        slot = slot + (src >= k * rows).astype(jnp.int32)
    node = src - slot * rows
    owner = jnp.zeros_like(src)
    for k in range(nbrs):
        owner = jnp.where(slot == k, nbr_ref[0, k], owner)
    distance = me_g - owner
    distance = jnp.where(distance < 0, distance + groups, distance)
    distance = jnp.where((slot < nbrs) & live, distance, -1)
    place = lax.broadcasted_iota(jnp.int32, (8, slots), 0)
    wanted = jnp.where(place < RADIUS, place + 1, groups - (place - (RADIUS - 1)))
    wanted = jnp.where(place < REACH, wanted, -2)
    from_place = (jnp.broadcast_to(distance, (8, slots)) == wanted).astype(F32)
    node_hot = (
        lax.broadcasted_iota(jnp.int32, (rows, slots), 0)
        == jnp.broadcast_to(node, (rows, slots))
    ).astype(F32).astype(BF16)
    uses = lax.dot_general(
        from_place.astype(BF16),
        node_hot,
        (((1,), (1,)), ((), ())),
        preferred_element_type=F32,
    )
    need = jnp.minimum(uses, 1.0)
    for p in range(REACH):
        ask[p] = jnp.broadcast_to(need[p : p + 1, :], (8, rows))

    pl.semaphore_wait(barrier, REACH + peers - 1)

    def ask_copy(p):
        return pltpu.make_async_remote_copy(
            src_ref=ask.at[p],
            dst_ref=asked.at[p],
            send_sem=ask_send.at[p],
            recv_sem=ask_recv.at[p],
            device_id=(ahead(-steps[p]), me_m),
            device_id_type=MESH,
        )

    for p in range(REACH):
        ask_copy(p).start()

    before = (
        lax.broadcasted_iota(jnp.int32, (rows, rows), 0)
        < lax.broadcasted_iota(jnp.int32, (rows, rows), 1)
    ).astype(F32).astype(BF16)

    loads[0].wait()
    loads[1].wait()
    states = x[...].reshape(members * rows, width)
    table[:, :rows, :] = (
        dot(states, ein[1]).astype(BF16).reshape(members, rows, width)
    )

    for p in range(REACH):
        ask_copy(p).wait_recv()
    picks = []
    for p in range(REACH):
        got = asked[p]
        rank = dot(got.astype(BF16), before)
        order = lax.broadcasted_iota(jnp.int32, (CAP, rows), 0).astype(F32)
        pick = (jnp.broadcast_to(rank[:1], (CAP, rows)) == order) & (
            jnp.broadcast_to(got[:1], (CAP, rows)) > 0.0
        )
        picks.append(pick.astype(F32).astype(BF16))
    picks = jnp.concatenate(picks, axis=0)

    def row_copy(m, p):
        return pltpu.make_async_remote_copy(
            src_ref=outbox.at[m, p],
            dst_ref=table.at[m, pl.ds(2 * rows + p * CAP, CAP)],
            send_sem=row_send.at[m, p],
            recv_sem=row_recv.at[m, p],
            device_id=(ahead(steps[p]), me_m),
            device_id_type=MESH,
        )

    for m in range(members):
        outbox[m] = dot(picks, table[m, :rows, :]).astype(BF16).reshape(REACH, CAP, width)
        for p in range(REACH):
            row_copy(m, p).start()

    loads[2].wait()
    table[:, rows : 2 * rows, :] = (
        dot(states, ein[2]).astype(BF16).reshape(members, rows, width)
    )
    tail = 2 * rows + REACH * CAP
    table[:, tail:, :] = jnp.zeros((members, table.shape[1] - tail, width), BF16)
    ranks = dot(need.astype(BF16), before).astype(BF16)
    rank = jnp.sum(dot(ranks, node_hot) * from_place, axis=0, keepdims=True)
    at_place = jnp.sum(from_place * place.astype(F32), axis=0, keepdims=True)
    target = jnp.where(
        slot == nbrs, node.astype(F32), 2.0 * rows + at_place * CAP + rank
    )
    lanes = 128
    target = jnp.broadcast_to(target, (lanes, slots)).T
    receiver = jnp.broadcast_to(dst.astype(F32) + rows, (lanes, slots)).T
    column = lax.broadcasted_iota(jnp.int32, (slots, lanes), 1).astype(F32)
    for s in range(table.shape[1] // lanes):
        column_s = column + float(s * lanes)
        hit = (target == column_s) | (receiver == column_s)
        hot[:, s * lanes : (s + 1) * lanes] = hit.astype(F32).astype(BF16)
    dest_hot[...] = (
        (
            lax.broadcasted_iota(jnp.int32, (rows, slots), 0)
            == jnp.broadcast_to(dst, (rows, slots))
        )
        & jnp.broadcast_to(live, (rows, slots))
    ).astype(F32).astype(BF16)
    loads[3].wait()
    loads[4].wait()
    edge_proj[...] = dot(edge[...], ein[0]) + bias_ref[0, 0:1, :]
    loads[5].wait()
    node_proj[...] = (dot(states, nin[0]) + bias_ref[0, 2:3, :]).reshape(
        members, rows, width
    )
    loads[6].wait()
    loads[7].wait()

    def fin_copy(m, k):
        return pltpu.make_async_remote_copy(
            src_ref=finals.at[m, pl.ds(pl.multiple_of(peer(k) * part, part), part)],
            dst_ref=inbox.at[k - 1, m],
            send_sem=fin_send.at[m, k - 1],
            recv_sem=fin_recv.at[m, k - 1],
            device_id=(me_g, peer(k)),
            device_id_type=MESH,
        )

    chunk = slots // 3

    def one_member(m, carry):
        for p in range(REACH):
            row_copy(m, p).wait_recv()
        total = jnp.zeros((rows, width), F32)
        for c in range(0, slots, chunk):
            hidden = dot(hot[c : c + chunk, :], table[m]) + edge_proj[c : c + chunk, :]
            mixed = dot(silu(hidden).astype(BF16), eout[...]) + bias_ref[0, 1:2, :]
            updated = edge[c : c + chunk, :].astype(F32) + layer_norm(
                mixed, gain_ref[0, 0:1, :]
            )
            total = total + dot(dest_hot[:, c : c + chunk], updated.astype(BF16))
        hidden = node_proj[m] + dot(total.astype(BF16), nin[1])
        mixed = dot(silu(hidden).astype(BF16), nout[...]) + bias_ref[0, 3:4, :]
        final = x[m].astype(F32) + layer_norm(mixed, gain_ref[0, 1:2, :])
        finals[m] = final.astype(BF16)
        for k in range(1, peers):
            fin_copy(m, k).start()
        return carry

    lax.fori_loop(0, members, one_member, 0)

    for m in range(members):
        for k in range(1, peers):
            fin_copy(m, k).wait_recv()
    mine = pl.ds(pl.multiple_of(me_m * part, part), part)
    ensemble = members * peers
    parts = [finals[m, mine, :] for m in range(members)]
    parts += [inbox[k, m] for k in range(peers - 1) for m in range(members)]
    total = parts[0].astype(F32)
    for value in parts[1:]:
        total = total + value.astype(F32)
    centre = total * (1.0 / ensemble)
    square = jnp.zeros_like(centre)
    for value in parts:
        deviation = value.astype(F32) - centre
        square = square + deviation * deviation
    out_ref[0, mine, :] = centre.astype(BF16)
    out_ref[1, mine, :] = jnp.sqrt(square * (1.0 / ensemble)).astype(BF16)

    def res_copy(i, k):
        return pltpu.make_async_remote_copy(
            src_ref=out_ref.at[i, mine],
            dst_ref=out_ref.at[i, mine],
            send_sem=res_send.at[i, k - 1],
            recv_sem=res_recv.at[i, k - 1],
            device_id=(me_g, peer(k)),
            device_id_type=MESH,
        )

    for k in range(1, peers):
        for i in range(2):
            res_copy(i, k).start()
    for k in range(1, peers):
        for i in range(2):
            res_copy(i, k).wait()
    for p in range(REACH):
        ask_copy(p).wait_send()
        for m in range(members):
            row_copy(m, p).wait_send()
    for k in range(1, peers):
        for m in range(members):
            fin_copy(m, k).wait_send()


def local(
    node_latents,
    edge_latents,
    neighbours,
    edge_source,
    edge_dest,
    edge_count,
    edge_in,
    edge_out,
    node_in,
    node_out,
    biases,
    gains,
):
    members, rows, width = node_latents.shape
    slots = edge_source.shape[1]
    groups = lax.axis_size("graph")
    peers = lax.axis_size("member")
    part = rows // peers
    depth = 2 * rows + -(-(REACH * CAP) // 256) * 256
    vmem = pl.BlockSpec(memory_space=pltpu.VMEM)
    smem = pl.BlockSpec(memory_space=pltpu.SMEM)
    hbm = pl.BlockSpec(memory_space=pl.ANY)
    dma = pltpu.SemaphoreType.DMA
    both = pl.pallas_call(
        functools.partial(kernel, groups, peers),
        out_shape=jax.ShapeDtypeStruct((2, rows, width), BF16),
        in_specs=[smem, smem] + [vmem] * 4 + [hbm] * 6,
        out_specs=vmem,
        scratch_shapes=[
            pltpu.VMEM((members, rows, width), BF16),
            pltpu.VMEM((slots, width), BF16),
            pltpu.VMEM((3, width, width), BF16),
            pltpu.VMEM((width, width), BF16),
            pltpu.VMEM((2, width, width), BF16),
            pltpu.VMEM((width, width), BF16),
            pltpu.VMEM((REACH, 8, rows), F32),
            pltpu.VMEM((REACH, 8, rows), F32),
            pltpu.VMEM((members, REACH, CAP, width), BF16),
            pltpu.VMEM((members, depth, width), BF16),
            pltpu.VMEM((slots, depth), BF16),
            pltpu.VMEM((rows, slots), BF16),
            pltpu.VMEM((slots, width), F32),
            pltpu.VMEM((members, rows, width), F32),
            pltpu.VMEM((members, rows, width), BF16),
            pltpu.VMEM((peers - 1, members, part, width), BF16),
            dma((8,)),
            dma((REACH,)),
            dma((REACH,)),
            dma((members, REACH)),
            dma((members, REACH)),
            dma((members, peers - 1)),
            dma((members, peers - 1)),
            dma((2, peers - 1)),
            dma((2, peers - 1)),
        ],
        compiler_params=pltpu.CompilerParams(collective_id=0, has_side_effects=True),
    )(
        neighbours,
        edge_count,
        edge_source,
        edge_dest,
        biases,
        gains,
        node_latents,
        edge_latents,
        edge_in,
        edge_out,
        node_in,
        node_out,
    )
    return (both[0], both[1])


def solution(mesh):
    return jax.shard_map(
        local,
        mesh=mesh,
        in_specs=(
            P("member", "graph", None),
            P("graph", None),
            P("graph", None),
            P("graph", None),
            P("graph", None),
            P("graph"),
            P(),
            P(),
            P(),
            P(),
            P(),
            P(),
        ),
        out_specs=(P("graph", None), P("graph", None)),
        check_vma=False,
    )
```

```python
import functools

import jax
import jax.numpy as jnp
from jax import lax
from jax.experimental import pallas as pl
from jax.experimental.pallas import tpu as pltpu
from jax.sharding import PartitionSpec as P

RADIUS = 3
CAP = 32
REACH = 2 * RADIUS
MESH = pl.DeviceIdType.MESH
F32 = jnp.float32
BF16 = jnp.bfloat16


def dot(a, b):
    return jnp.dot(a, b, preferred_element_type=F32)


def silu(v):
    h = 0.5 * v
    return h * jnp.tanh(h) + h


def layer_norm(values, gain):
    centre = jnp.mean(values, axis=-1, keepdims=True)
    centered = values - centre
    variance = jnp.mean(centered * centered, axis=-1, keepdims=True)
    return centered * lax.rsqrt(variance + 1e-05) * gain


def kernel(
    groups,
    peers,
    nbr_ref,
    count_ref,
    src_ref,
    dst_ref,
    bias_ref,
    gain_ref,
    x_hbm,
    edge_hbm,
    ein_hbm,
    eout_hbm,
    nin_hbm,
    nout_hbm,
    out_ref,
    x,
    edge,
    ein,
    eout,
    nin,
    nout,
    ask,
    asked,
    outbox,
    table,
    hot,
    dest_hot,
    edge_proj,
    node_proj,
    finals,
    inbox,
    load_sem,
    ask_send,
    ask_recv,
    row_send,
    row_recv,
    fin_send,
    fin_recv,
    res_send,
    res_recv,
):
    members, rows, width = x.shape
    slots = edge.shape[0]
    nbrs = nbr_ref.shape[1]
    part = inbox.shape[2]
    pair = rows // part
    me_g = lax.axis_index("graph")
    me_m = lax.axis_index("member")
    steps = [r + 1 for r in range(RADIUS)] + [-(r + 1) for r in range(RADIUS)]

    def ahead(step):
        return lax.rem(me_g + step + groups, groups)

    def peer(k):
        return lax.rem(me_m + k, peers)

    loads = [
        pltpu.make_async_copy(s, d, load_sem.at[i])
        for i, (s, d) in enumerate(
            [
                (x_hbm, x),
                (ein_hbm.at[0, 1], ein.at[1]),
                (ein_hbm.at[0, 2], ein.at[2]),
                (edge_hbm, edge),
                (ein_hbm.at[0, 0], ein.at[0]),
                (nin_hbm.at[0], nin),
                (eout_hbm.at[0], eout),
                (nout_hbm.at[0], nout),
            ]
        )
    ]
    for load in loads:
        load.start()

    barrier = pltpu.get_barrier_semaphore()
    for step in steps:
        pl.semaphore_signal(
            barrier, inc=1, device_id=(ahead(step), me_m), device_id_type=MESH
        )
    for k in range(1, peers):
        pl.semaphore_signal(
            barrier, inc=1, device_id=(me_g, peer(k)), device_id_type=MESH
        )

    src = src_ref[...]
    dst = dst_ref[...]
    live = lax.broadcasted_iota(jnp.int32, (1, slots), 1) < count_ref[0]
    slot = jnp.zeros_like(src)
    for k in range(1, nbrs + 1):
        slot = slot + (src >= k * rows).astype(jnp.int32)
    node = src - slot * rows
    owner = jnp.zeros_like(src)
    for k in range(nbrs):
        owner = jnp.where(slot == k, nbr_ref[0, k], owner)
    distance = me_g - owner
    distance = jnp.where(distance < 0, distance + groups, distance)
    distance = jnp.where((slot < nbrs) & live, distance, -1)
    place = lax.broadcasted_iota(jnp.int32, (8, slots), 0)
    wanted = jnp.where(place < RADIUS, place + 1, groups - (place - (RADIUS - 1)))
    wanted = jnp.where(place < REACH, wanted, -2)
    from_place = (jnp.broadcast_to(distance, (8, slots)) == wanted).astype(F32)
    node_hot = (
        lax.broadcasted_iota(jnp.int32, (rows, slots), 0)
        == jnp.broadcast_to(node, (rows, slots))
    ).astype(F32).astype(BF16)
    uses = lax.dot_general(
        from_place.astype(BF16),
        node_hot,
        (((1,), (1,)), ((), ())),
        preferred_element_type=F32,
    )
    need = jnp.minimum(uses, 1.0)
    for p in range(REACH):
        ask[p] = jnp.broadcast_to(need[p : p + 1, :], (8, rows))

    pl.semaphore_wait(barrier, REACH + peers - 1)

    def ask_copy(p):
        return pltpu.make_async_remote_copy(
            src_ref=ask.at[p],
            dst_ref=asked.at[p],
            send_sem=ask_send.at[p],
            recv_sem=ask_recv.at[p],
            device_id=(ahead(-steps[p]), me_m),
            device_id_type=MESH,
        )

    for p in range(REACH):
        ask_copy(p).start()

    before = (
        lax.broadcasted_iota(jnp.int32, (rows, rows), 0)
        < lax.broadcasted_iota(jnp.int32, (rows, rows), 1)
    ).astype(F32).astype(BF16)

    loads[0].wait()
    loads[1].wait()
    states = x[...].reshape(members * rows, width)
    table[:, :rows, :] = (
        dot(states, ein[1]).astype(BF16).reshape(members, rows, width)
    )

    for p in range(REACH):
        ask_copy(p).wait_recv()
    picks = []
    for p in range(REACH):
        got = asked[p]
        rank = dot(got.astype(BF16), before)
        order = lax.broadcasted_iota(jnp.int32, (CAP, rows), 0).astype(F32)
        pick = (jnp.broadcast_to(rank[:1], (CAP, rows)) == order) & (
            jnp.broadcast_to(got[:1], (CAP, rows)) > 0.0
        )
        picks.append(pick.astype(F32).astype(BF16))
    picks = jnp.concatenate(picks, axis=0)

    def row_copy(m, p):
        return pltpu.make_async_remote_copy(
            src_ref=outbox.at[m, p],
            dst_ref=table.at[m, pl.ds(2 * rows + p * CAP, CAP)],
            send_sem=row_send.at[m, p],
            recv_sem=row_recv.at[m, p],
            device_id=(ahead(steps[p]), me_m),
            device_id_type=MESH,
        )

    for m in range(members):
        outbox[m] = dot(picks, table[m, :rows, :]).astype(BF16).reshape(REACH, CAP, width)
        for p in range(REACH):
            row_copy(m, p).start()

    loads[2].wait()
    table[:, rows : 2 * rows, :] = (
        dot(states, ein[2]).astype(BF16).reshape(members, rows, width)
    )
    tail = 2 * rows + REACH * CAP
    table[:, tail:, :] = jnp.zeros((members, table.shape[1] - tail, width), BF16)
    ranks = dot(need.astype(BF16), before).astype(BF16)
    rank = jnp.sum(dot(ranks, node_hot) * from_place, axis=0, keepdims=True)
    at_place = jnp.sum(from_place * place.astype(F32), axis=0, keepdims=True)
    target = jnp.where(
        slot == nbrs, node.astype(F32), 2.0 * rows + at_place * CAP + rank
    )
    lanes = 128
    target = jnp.broadcast_to(target, (lanes, slots)).T
    receiver = jnp.broadcast_to(dst.astype(F32) + rows, (lanes, slots)).T
    column = lax.broadcasted_iota(jnp.int32, (slots, lanes), 1).astype(F32)
    for s in range(table.shape[1] // lanes):
        column_s = column + float(s * lanes)
        hit = (target == column_s) | (receiver == column_s)
        hot[:, s * lanes : (s + 1) * lanes] = hit.astype(F32).astype(BF16)
    dest_hot[...] = (
        (
            lax.broadcasted_iota(jnp.int32, (rows, slots), 0)
            == jnp.broadcast_to(dst, (rows, slots))
        )
        & jnp.broadcast_to(live, (rows, slots))
    ).astype(F32).astype(BF16)
    loads[3].wait()
    loads[4].wait()
    edge_proj[...] = dot(edge[...], ein[0]) + bias_ref[0, 0:1, :]
    loads[5].wait()
    node_proj[...] = (dot(states, nin[0]) + bias_ref[0, 2:3, :]).reshape(
        members, rows, width
    )
    loads[6].wait()
    loads[7].wait()

    def share(device):
        return pl.ds(pl.multiple_of(lax.rem(device, pair) * part, part), part)

    def fin_copy(m, k):
        return pltpu.make_async_remote_copy(
            src_ref=finals.at[m, share(peer(k))],
            dst_ref=inbox.at[k - 1, m],
            send_sem=fin_send.at[m, k - 1],
            recv_sem=fin_recv.at[m, k - 1],
            device_id=(me_g, peer(k)),
            device_id_type=MESH,
        )

    chunk = slots // 3

    def one_member(m, carry):
        for p in range(REACH):
            row_copy(m, p).wait_recv()
        total = jnp.zeros((rows, width), F32)
        for c in range(0, slots, chunk):
            hidden = dot(hot[c : c + chunk, :], table[m]) + edge_proj[c : c + chunk, :]
            mixed = dot(silu(hidden).astype(BF16), eout[...]) + bias_ref[0, 1:2, :]
            updated = edge[c : c + chunk, :].astype(F32) + layer_norm(
                mixed, gain_ref[0, 0:1, :]
            )
            total = total + dot(dest_hot[:, c : c + chunk], updated.astype(BF16))
        hidden = node_proj[m] + dot(total.astype(BF16), nin[1])
        mixed = dot(silu(hidden).astype(BF16), nout[...]) + bias_ref[0, 3:4, :]
        final = x[m].astype(F32) + layer_norm(mixed, gain_ref[0, 1:2, :])
        finals[m] = final.astype(BF16)
        for k in range(1, peers):
            fin_copy(m, k).start()
        return carry

    lax.fori_loop(0, members, one_member, 0)

    for m in range(members):
        for k in range(1, peers):
            fin_copy(m, k).wait_recv()
    mine = share(me_m)
    first = me_m - lax.rem(me_m, pair)
    ensemble = members * peers
    parts = [finals[m, mine, :] for m in range(members)]
    parts += [inbox[k, m] for k in range(peers - 1) for m in range(members)]
    total = parts[0].astype(F32)
    for value in parts[1:]:
        total = total + value.astype(F32)
    centre = total * (1.0 / ensemble)
    square = jnp.zeros_like(centre)
    for value in parts:
        deviation = value.astype(F32) - centre
        square = square + deviation * deviation
    out_ref[0, mine, :] = centre.astype(BF16)
    out_ref[1, mine, :] = jnp.sqrt(square * (1.0 / ensemble)).astype(BF16)

    def mate(k):
        return first + lax.rem(me_m - first + k, pair)

    def res_copy(i, k):
        return pltpu.make_async_remote_copy(
            src_ref=out_ref.at[i, mine],
            dst_ref=out_ref.at[i, mine],
            send_sem=res_send.at[i, k - 1],
            recv_sem=res_recv.at[i, k - 1],
            device_id=(me_g, mate(k)),
            device_id_type=MESH,
        )

    for k in range(1, pair):
        for i in range(2):
            res_copy(i, k).start()
    for k in range(1, pair):
        for i in range(2):
            res_copy(i, k).wait()
    for p in range(REACH):
        ask_copy(p).wait_send()
        for m in range(members):
            row_copy(m, p).wait_send()
    for k in range(1, peers):
        for m in range(members):
            fin_copy(m, k).wait_send()


def local(
    node_latents,
    edge_latents,
    neighbours,
    edge_source,
    edge_dest,
    edge_count,
    edge_in,
    edge_out,
    node_in,
    node_out,
    biases,
    gains,
):
    members, rows, width = node_latents.shape
    slots = edge_source.shape[1]
    groups = lax.axis_size("graph")
    peers = lax.axis_size("member")
    pair = 2 - peers % 2
    part = rows // pair
    depth = 2 * rows + -(-(REACH * CAP) // 256) * 256
    vmem = pl.BlockSpec(memory_space=pltpu.VMEM)
    smem = pl.BlockSpec(memory_space=pltpu.SMEM)
    hbm = pl.BlockSpec(memory_space=pl.ANY)
    dma = pltpu.SemaphoreType.DMA
    both = pl.pallas_call(
        functools.partial(kernel, groups, peers),
        out_shape=jax.ShapeDtypeStruct((2, rows, width), BF16),
        in_specs=[smem, smem] + [vmem] * 4 + [hbm] * 6,
        out_specs=vmem,
        scratch_shapes=[
            pltpu.VMEM((members, rows, width), BF16),
            pltpu.VMEM((slots, width), BF16),
            pltpu.VMEM((3, width, width), BF16),
            pltpu.VMEM((width, width), BF16),
            pltpu.VMEM((2, width, width), BF16),
            pltpu.VMEM((width, width), BF16),
            pltpu.VMEM((REACH, 8, rows), F32),
            pltpu.VMEM((REACH, 8, rows), F32),
            pltpu.VMEM((members, REACH, CAP, width), BF16),
            pltpu.VMEM((members, depth, width), BF16),
            pltpu.VMEM((slots, depth), BF16),
            pltpu.VMEM((rows, slots), BF16),
            pltpu.VMEM((slots, width), F32),
            pltpu.VMEM((members, rows, width), F32),
            pltpu.VMEM((members, rows, width), BF16),
            pltpu.VMEM((peers - 1, members, part, width), BF16),
            dma((8,)),
            dma((REACH,)),
            dma((REACH,)),
            dma((members, REACH)),
            dma((members, REACH)),
            dma((members, peers - 1)),
            dma((members, peers - 1)),
            dma((2, pair)),
            dma((2, pair)),
        ],
        compiler_params=pltpu.CompilerParams(collective_id=0, has_side_effects=True),
    )(
        neighbours,
        edge_count,
        edge_source,
        edge_dest,
        biases,
        gains,
        node_latents,
        edge_latents,
        edge_in,
        edge_out,
        node_in,
        node_out,
    )
    return (both[0], both[1])


def solution(mesh):
    return jax.shard_map(
        local,
        mesh=mesh,
        in_specs=(
            P("member", "graph", None),
            P("graph", None),
            P("graph", None),
            P("graph", None),
            P("graph", None),
            P("graph"),
            P(),
            P(),
            P(),
            P(),
            P(),
            P(),
        ),
        out_specs=(P("graph", None), P("graph", None)),
        check_vma=False,
    )
```

```python
import functools

import jax
import jax.numpy as jnp
from jax import lax
from jax.experimental import pallas as pl
from jax.experimental.pallas import tpu as pltpu
from jax.sharding import PartitionSpec as P

RADIUS = 3
CAP = 32
REACH = 2 * RADIUS
WAVES = ((0, 1, 2, 3, 4, 5),)
MESH = pl.DeviceIdType.MESH
F32 = jnp.float32
BF16 = jnp.bfloat16


def dot(a, b):
    return jnp.dot(a, b, preferred_element_type=F32)


def silu(v):
    h = 0.5 * v
    return h * jnp.tanh(h) + h


def layer_norm(values, gain):
    centre = jnp.mean(values, axis=-1, keepdims=True)
    centered = values - centre
    variance = jnp.mean(centered * centered, axis=-1, keepdims=True)
    return centered * lax.rsqrt(variance + 1e-05) * gain


def kernel(
    groups,
    peers,
    nbr_ref,
    count_ref,
    src_ref,
    dst_ref,
    bias_ref,
    gain_ref,
    x_hbm,
    edge_hbm,
    ein_hbm,
    eout_hbm,
    nin_hbm,
    nout_hbm,
    out_ref,
    x,
    edge,
    ein,
    eout,
    nin,
    nout,
    ask,
    asked,
    outbox,
    table,
    hot,
    dest_hot,
    edge_proj,
    node_proj,
    finals,
    inbox,
    load_sem,
    ask_send,
    ask_recv,
    row_send,
    row_recv,
    fin_send,
    fin_recv,
    res_send,
    res_recv,
):
    members, rows, width = x.shape
    slots = edge.shape[0]
    nbrs = nbr_ref.shape[1]
    part = inbox.shape[2]
    pair = rows // part
    me_g = lax.axis_index("graph")
    me_m = lax.axis_index("member")
    steps = [r + 1 for r in range(RADIUS)] + [-(r + 1) for r in range(RADIUS)]

    def ahead(step):
        return lax.rem(me_g + step + groups, groups)

    def peer(k):
        return lax.rem(me_m + k, peers)

    loads = [
        pltpu.make_async_copy(s, d, load_sem.at[i])
        for i, (s, d) in enumerate(
            [
                (x_hbm, x),
                (ein_hbm.at[0, 1], ein.at[1]),
                (ein_hbm.at[0, 2], ein.at[2]),
                (edge_hbm, edge),
                (ein_hbm.at[0, 0], ein.at[0]),
                (nin_hbm.at[0], nin),
                (eout_hbm.at[0], eout),
                (nout_hbm.at[0], nout),
            ]
        )
    ]
    barrier = pltpu.get_barrier_semaphore()
    for step in steps:
        pl.semaphore_signal(
            barrier, inc=1, device_id=(ahead(step), me_m), device_id_type=MESH
        )
    for k in range(1, peers):
        pl.semaphore_signal(
            barrier, inc=1, device_id=(me_g, peer(k)), device_id_type=MESH
        )

    for load in loads:
        load.start()

    src = src_ref[...]
    dst = dst_ref[...]
    live = lax.broadcasted_iota(jnp.int32, (1, slots), 1) < count_ref[0, 0]
    slot = jnp.zeros_like(src)
    for k in range(1, nbrs + 1):
        slot = slot + (src >= k * rows).astype(jnp.int32)
    node = src - slot * rows
    owner = jnp.zeros_like(src)
    for k in range(nbrs):
        owner = jnp.where(slot == k, nbr_ref[0, k], owner)
    distance = me_g - owner
    distance = jnp.where(distance < 0, distance + groups, distance)
    distance = jnp.where((slot < nbrs) & live, distance, -1)
    place = lax.broadcasted_iota(jnp.int32, (8, slots), 0)
    wanted = jnp.where(place < RADIUS, place + 1, groups - (place - (RADIUS - 1)))
    wanted = jnp.where(place < REACH, wanted, -2)
    from_place = (jnp.broadcast_to(distance, (8, slots)) == wanted).astype(F32)
    node_hot = (
        lax.broadcasted_iota(jnp.int32, (rows, slots), 0)
        == jnp.broadcast_to(node, (rows, slots))
    ).astype(F32).astype(BF16)
    uses = lax.dot_general(
        from_place.astype(BF16),
        node_hot,
        (((1,), (1,)), ((), ())),
        preferred_element_type=F32,
    )
    need = jnp.minimum(uses, 1.0)
    for p in range(REACH):
        ask[p] = jnp.broadcast_to(need[p : p + 1, :], (8, rows))

    pl.semaphore_wait(barrier, REACH + peers - 1)

    def ask_copy(p):
        return pltpu.make_async_remote_copy(
            src_ref=ask.at[p],
            dst_ref=asked.at[p],
            send_sem=ask_send.at[p],
            recv_sem=ask_recv.at[p],
            device_id=(ahead(-steps[p]), me_m),
            device_id_type=MESH,
        )

    for p in range(REACH):
        ask_copy(p).start()

    before = (
        lax.broadcasted_iota(jnp.int32, (rows, rows), 0)
        < lax.broadcasted_iota(jnp.int32, (rows, rows), 1)
    ).astype(F32).astype(BF16)

    loads[0].wait()
    loads[1].wait()
    states = x[...].reshape(members * rows, width)
    table[:, :rows, :] = (
        dot(states, ein[1]).astype(BF16).reshape(members, rows, width)
    )

    def picked(p):
        ask_copy(p).wait_recv()
        got = asked[p]
        rank = dot(got.astype(BF16), before)
        order = lax.broadcasted_iota(jnp.int32, (CAP, rows), 0).astype(F32)
        pick = (jnp.broadcast_to(rank[:1], (CAP, rows)) == order) & (
            jnp.broadcast_to(got[:1], (CAP, rows)) > 0.0
        )
        return pick.astype(F32).astype(BF16)

    def row_copy(m, p):
        return pltpu.make_async_remote_copy(
            src_ref=outbox.at[m, p],
            dst_ref=table.at[m, pl.ds(2 * rows + p * CAP, CAP)],
            send_sem=row_send.at[m, p],
            recv_sem=row_recv.at[m, p],
            device_id=(ahead(steps[p]), me_m),
            device_id_type=MESH,
        )

    for places in WAVES:
        picks = jnp.concatenate([picked(p) for p in places], axis=0)
        for m in range(members):
            drawn = dot(picks, table[m, :rows, :]).astype(BF16)
            for i, p in enumerate(places):
                outbox[m, p] = drawn[i * CAP : (i + 1) * CAP]
                row_copy(m, p).start()

    loads[2].wait()
    table[:, rows : 2 * rows, :] = (
        dot(states, ein[2]).astype(BF16).reshape(members, rows, width)
    )
    tail = 2 * rows + REACH * CAP
    table[:, tail:, :] = jnp.zeros((members, table.shape[1] - tail, width), BF16)
    ranks = dot(need.astype(BF16), before).astype(BF16)
    rank = jnp.sum(dot(ranks, node_hot) * from_place, axis=0, keepdims=True)
    at_place = jnp.sum(from_place * place.astype(F32), axis=0, keepdims=True)
    target = jnp.where(
        slot == nbrs, node.astype(F32), 2.0 * rows + at_place * CAP + rank
    )
    lanes = 128
    target = jnp.broadcast_to(target, (lanes, slots)).T
    receiver = jnp.broadcast_to(dst.astype(F32) + rows, (lanes, slots)).T
    column = lax.broadcasted_iota(jnp.int32, (slots, lanes), 1).astype(F32)
    for s in range(table.shape[1] // lanes):
        column_s = column + float(s * lanes)
        hit = (target == column_s) | (receiver == column_s)
        hot[:, s * lanes : (s + 1) * lanes] = hit.astype(F32).astype(BF16)
    dest_hot[...] = (
        (
            lax.broadcasted_iota(jnp.int32, (rows, slots), 0)
            == jnp.broadcast_to(dst, (rows, slots))
        )
        & jnp.broadcast_to(live, (rows, slots))
    ).astype(F32).astype(BF16)
    loads[3].wait()
    loads[4].wait()
    edge_proj[...] = dot(edge[...], ein[0]) + bias_ref[0, 0:1, :]
    loads[5].wait()
    node_proj[...] = (dot(states, nin[0]) + bias_ref[0, 2:3, :]).reshape(
        members, rows, width
    )
    loads[6].wait()
    loads[7].wait()

    def share(device):
        return pl.ds(pl.multiple_of(lax.rem(device, pair) * part, part), part)

    def fin_copy(m, k):
        return pltpu.make_async_remote_copy(
            src_ref=finals.at[m, share(peer(k))],
            dst_ref=inbox.at[k - 1, m],
            send_sem=fin_send.at[m, k - 1],
            recv_sem=fin_recv.at[m, k - 1],
            device_id=(me_g, peer(k)),
            device_id_type=MESH,
        )

    chunk = slots

    def one_member(m, carry):
        for p in range(REACH):
            row_copy(m, p).wait_recv()
        total = jnp.zeros((rows, width), F32)
        for c in range(0, slots, chunk):
            hidden = dot(hot[c : c + chunk, :], table[m]) + edge_proj[c : c + chunk, :]
            mixed = dot(silu(hidden).astype(BF16), eout[...]) + bias_ref[0, 1:2, :]
            updated = edge[c : c + chunk, :].astype(F32) + layer_norm(
                mixed, gain_ref[0, 0:1, :]
            )
            total = total + dot(dest_hot[:, c : c + chunk], updated.astype(BF16))
        hidden = node_proj[m] + dot(total.astype(BF16), nin[1])
        mixed = dot(silu(hidden).astype(BF16), nout[...]) + bias_ref[0, 3:4, :]
        final = x[m].astype(F32) + layer_norm(mixed, gain_ref[0, 1:2, :])
        finals[m] = final.astype(BF16)
        for k in range(1, peers):
            fin_copy(m, k).start()
        return carry

    lax.fori_loop(0, members, one_member, 0)

    for m in range(members):
        for k in range(1, peers):
            fin_copy(m, k).wait_recv()
    mine = share(me_m)
    first = me_m - lax.rem(me_m, pair)
    ensemble = members * peers
    parts = [finals[m, mine, :] for m in range(members)]
    parts += [inbox[k, m] for k in range(peers - 1) for m in range(members)]
    total = parts[0].astype(F32)
    for value in parts[1:]:
        total = total + value.astype(F32)
    centre = total * (1.0 / ensemble)
    square = jnp.zeros_like(centre)
    for value in parts:
        deviation = value.astype(F32) - centre
        square = square + deviation * deviation
    out_ref[0, mine, :] = centre.astype(BF16)
    out_ref[1, mine, :] = jnp.sqrt(square * (1.0 / ensemble)).astype(BF16)

    def mate(k):
        return first + lax.rem(me_m - first + k, pair)

    def res_copy(i, k):
        return pltpu.make_async_remote_copy(
            src_ref=out_ref.at[i, mine],
            dst_ref=out_ref.at[i, mine],
            send_sem=res_send.at[i, k - 1],
            recv_sem=res_recv.at[i, k - 1],
            device_id=(me_g, mate(k)),
            device_id_type=MESH,
        )

    for k in range(1, pair):
        for i in range(2):
            res_copy(i, k).start()
    for k in range(1, pair):
        for i in range(2):
            res_copy(i, k).wait()
    for p in range(REACH):
        ask_copy(p).wait_send()
        for m in range(members):
            row_copy(m, p).wait_send()
    for k in range(1, peers):
        for m in range(members):
            fin_copy(m, k).wait_send()


def local(
    node_latents,
    edge_latents,
    neighbours,
    edge_source,
    edge_dest,
    edge_count,
    edge_in,
    edge_out,
    node_in,
    node_out,
    biases,
    gains,
):
    members, rows, width = node_latents.shape
    slots = edge_source.shape[1]
    groups = lax.axis_size("graph")
    peers = lax.axis_size("member")
    pair = 2 - peers % 2
    part = rows // pair
    depth = 2 * rows + -(-(REACH * CAP) // 256) * 256
    vmem = pl.BlockSpec(memory_space=pltpu.VMEM)
    smem = pl.BlockSpec(memory_space=pltpu.SMEM)
    hbm = pl.BlockSpec(memory_space=pl.ANY)
    dma = pltpu.SemaphoreType.DMA
    both = pl.pallas_call(
        functools.partial(kernel, groups, peers),
        out_shape=jax.ShapeDtypeStruct((2, rows, width), BF16),
        in_specs=[smem, smem] + [vmem] * 4 + [hbm] * 6,
        out_specs=vmem,
        scratch_shapes=[
            pltpu.VMEM((members, rows, width), BF16),
            pltpu.VMEM((slots, width), BF16),
            pltpu.VMEM((3, width, width), BF16),
            pltpu.VMEM((width, width), BF16),
            pltpu.VMEM((2, width, width), BF16),
            pltpu.VMEM((width, width), BF16),
            pltpu.VMEM((REACH, 8, rows), F32),
            pltpu.VMEM((REACH, 8, rows), F32),
            pltpu.VMEM((members, REACH, CAP, width), BF16),
            pltpu.VMEM((members, depth, width), BF16),
            pltpu.VMEM((slots, depth), BF16),
            pltpu.VMEM((rows, slots), BF16),
            pltpu.VMEM((slots, width), F32),
            pltpu.VMEM((members, rows, width), F32),
            pltpu.VMEM((members, rows, width), BF16),
            pltpu.VMEM((peers - 1, members, part, width), BF16),
            dma((8,)),
            dma((REACH,)),
            dma((REACH,)),
            dma((members, REACH)),
            dma((members, REACH)),
            dma((members, peers - 1)),
            dma((members, peers - 1)),
            dma((2, pair)),
            dma((2, pair)),
        ],
        compiler_params=pltpu.CompilerParams(collective_id=0, has_side_effects=True),
    )(
        neighbours,
        edge_count.reshape(1, 1),
        edge_source,
        edge_dest,
        biases,
        gains,
        node_latents,
        edge_latents,
        edge_in,
        edge_out,
        node_in,
        node_out,
    )
    return (both[0], both[1])


def solution(mesh):
    return jax.shard_map(
        local,
        mesh=mesh,
        in_specs=(
            P("member", "graph", None),
            P("graph", None),
            P("graph", None),
            P("graph", None),
            P("graph", None),
            P("graph"),
            P(),
            P(),
            P(),
            P(),
            P(),
            P(),
        ),
        out_specs=(P("graph", None), P("graph", None)),
        check_vma=False,
    )
```
